32 devices in a mesh: blk: 8 (over y, x, core), heads: 4 (over z).
Axes of the slice: x: 2, y: 2, z: 4, core: 2. Of those that a mesh axis runs over, the one named last changes fastest.
Arguments:
- queries: bfloat16 [2048, 4096], P('blk', 'heads'), may hold values from -5 to 5
- keys: bfloat16 [2048, 1024], P('blk', 'heads'), may hold values from -5 to 5
- values: bfloat16 [2048, 1024], P('blk', 'heads'), may hold values from -6 to 6
- doc_ids: int32 [2048], P('blk'), may hold values from 0 to 7, never falling along the last dimension, each value on 1 to 1024 neighbouring positions
Outputs:
- attended: bfloat16 [2048, 4096], P('blk', 'heads')
The draws below stay inside these ranges and needn't reach their ends.
Inputs may be any that keep to these rules, and one draw needn't show every extreme that they name: `doc_ids`: Non-decreasing along the sequence; every document has 1024 tokens at most, and some document exactly 1024.
All inputs are finite; a program needn't handle non-finite values.
Results may differ from the reference program's by a relative error of at most 0.0034.
Values may be sent and summed in bfloat16 or wider, within the bound.
A program may use at most 64 MiB of HBM per device.

```python
import math
import jax
import jax.numpy as jnp
import numpy as np
from jax import lax

QUERY_HEAD_COUNT = 32
KEY_VALUE_HEADS = 8
HEAD_WIDTH = 128
BLOCK_TOKENS = 256
DOC_BLKS = 4
MAXDOC = 1024
PACKED_TOKENS = 2048
DOCS = 8


def make_pair(key):
    start_offset = jax.random.fold_in(key, 7)
    key_portion = jnp.clip(jax.random.normal(jax.random.fold_in(start_offset, 1), (PACKED_TOKENS, KEY_VALUE_HEADS * HEAD_WIDTH), jnp.float32), -4.0, 4.0)
    query_part = jnp.clip(jax.random.normal(jax.random.fold_in(start_offset, 2), (PACKED_TOKENS, QUERY_HEAD_COUNT * HEAD_WIDTH), jnp.float32), -4.0, 4.0)
    return (query_part, key_portion)


def draw_queries(key, part):
    return make_pair(key)[0].astype(jnp.bfloat16)


def draw_keys(key, part):
    return make_pair(key)[1].astype(jnp.bfloat16)


def block_levels(own_key, shape, cuts, smallest, high):
    loudness = 1.0
    for dim, parts in cuts:
        draws = jax.random.uniform(jax.random.fold_in(jax.random.fold_in(own_key, 6), dim), (parts,), jnp.float32, smallest / len(cuts), high / len(cuts))
        loudness = loudness * jnp.repeat(jnp.exp(draws), shape[dim] // parts).reshape((-1,) + (1,) * (len(shape) - 1 - dim))
    return loudness


def profile(count, total, limit, slope):
    loads = [(1 << 20) // math.isqrt(standing ** slope) + 1 for standing in range(2, count + 1)]
    surplus, counts = total - limit - (count - 1), [1] * (count - 1)
    while surplus > 0:
        movable = [i for i in range(count - 1) if counts[i] < limit]
        whole, left = sum([loads[i] for i in movable]), surplus
        for i in movable:
            addition = min(limit - counts[i], max(1, left * loads[i] // whole), surplus)
            counts[i] = counts[i] + addition
            surplus = surplus - addition
    return np.array([limit] + counts)


def ragged_sizes(stream_key, count, total, most, slope):
    if count == 2:
        one = jax.random.randint(stream_key, (), max(1, total - most), min(most, total - 1) + 1)
        return jnp.stack([one, total - one])
    sizes = jnp.asarray(profile(count, total, most, slope), jnp.int32)
    twos = (count - 1) // 2
    source_of, taker = sizes[1:1 + 2 * twos:2], sizes[2:2 + 2 * twos:2]
    room = jnp.minimum(source_of - 1, most - taker)
    shifted = jax.random.randint(jax.random.fold_in(stream_key, 1), (twos,), 0, 1 << 20) % (room + 1)
    sizes = sizes.at[1:1 + 2 * twos:2].set(source_of - shifted).at[2:2 + 2 * twos:2].set(taker + shifted)
    return sizes[jax.random.permutation(jax.random.fold_in(stream_key, 2), count)]


def gaussian(own_key, dims, spread, most, split=(), held_as=jnp.bfloat16):
    array = jax.random.normal(own_key, dims, jnp.float32) * spread
    if len(split) > 0:
        array = block_levels(own_key, dims, split, -0.22, 0.18) * array
    return jnp.clip(array, min=-most, max=most).astype(held_as)


def setup_inputs(seed: int = 0) -> dict:
    arg_keys = jax.random.split(jax.random.key(seed), 5)
    return {
        "queries": draw_queries(jax.random.fold_in(arg_keys[4], 71), 0),
        "keys": draw_keys(jax.random.fold_in(arg_keys[4], 71), 0),
        "values": gaussian(arg_keys[2], (PACKED_TOKENS, KEY_VALUE_HEADS * HEAD_WIDTH), 1.0, 6.0, ((0, 8), (1, 4))),
        "doc_ids": jnp.searchsorted(jnp.cumsum(ragged_sizes(arg_keys[3], DOCS, PACKED_TOKENS, MAXDOC, 2)), jnp.arange(PACKED_TOKENS), side="right").astype(jnp.int32),
    }


def reference(queries, keys, values, doc_ids):
    seq_length = queries.shape[0]
    backward_extent = DOC_BLKS * BLOCK_TOKENS
    visible_span = backward_extent + BLOCK_TOKENS
    queries_per_group = QUERY_HEAD_COUNT // KEY_VALUE_HEADS
    score_scale = 1.0 / math.sqrt(HEAD_WIDTH)
    padded_key_rows = jnp.concatenate([jnp.zeros((backward_extent, KEY_VALUE_HEADS * HEAD_WIDTH), keys.dtype), keys], axis=0)
    padded_value_rows = jnp.concatenate([jnp.zeros((backward_extent, KEY_VALUE_HEADS * HEAD_WIDTH), values.dtype), values], axis=0)
    docs_padded = jnp.concatenate([-jnp.ones((backward_extent,), jnp.int32), doc_ids.astype(jnp.int32)], axis=0)

    def one_block(block_index):
        first_row = (block_index * BLOCK_TOKENS).astype(jnp.int32)
        block_of_queries = lax.dynamic_slice_in_dim(queries, first_row, BLOCK_TOKENS, 0)
        block_of_queries = block_of_queries.reshape(BLOCK_TOKENS, KEY_VALUE_HEADS, queries_per_group, HEAD_WIDTH).astype(jnp.float32)
        block_of_keys = lax.dynamic_slice_in_dim(padded_key_rows, first_row, visible_span, 0)
        block_of_keys = block_of_keys.reshape(visible_span, KEY_VALUE_HEADS, HEAD_WIDTH).astype(jnp.float32)
        block_of_values = lax.dynamic_slice_in_dim(padded_value_rows, first_row, visible_span, 0)
        block_of_values = block_of_values.reshape(visible_span, KEY_VALUE_HEADS, HEAD_WIDTH).astype(jnp.float32)
        query_docs = lax.dynamic_slice_in_dim(doc_ids.astype(jnp.int32), first_row, BLOCK_TOKENS, 0)
        key_docs = lax.dynamic_slice_in_dim(docs_padded, first_row, visible_span, 0)
        query_pos = first_row + jnp.arange(BLOCK_TOKENS, dtype=jnp.int32)
        key_pos = first_row - backward_extent + jnp.arange(visible_span, dtype=jnp.int32)
        allowed = (query_docs[:, None] == key_docs[None, :]) & (key_pos[None, :] <= query_pos[:, None])
        scores = jnp.einsum('qkgd,skd->kgqs', block_of_queries, block_of_keys) * score_scale
        scores = jnp.where(allowed, scores, -jnp.inf)
        rowmax = lax.optimization_barrier(jnp.max(scores, axis=-1, keepdims=True))
        weights = jnp.exp(scores - rowmax)
        denominator = lax.optimization_barrier(jnp.sum(weights, axis=-1))
        rounded = lax.optimization_barrier(weights.astype(jnp.bfloat16)).astype(jnp.float32)
        numerator = jnp.einsum('kgqs,skd->qkgd', rounded, block_of_values)
        result = numerator / jnp.transpose(denominator, (2, 0, 1))[..., None]
        return result.reshape(BLOCK_TOKENS, QUERY_HEAD_COUNT * HEAD_WIDTH).astype(jnp.bfloat16)
    blocks_out = lax.map(one_block, jnp.arange(seq_length // BLOCK_TOKENS, dtype=jnp.int32))
    return blocks_out.reshape(seq_length, QUERY_HEAD_COUNT * HEAD_WIDTH)
```

```python
import functools
import math

import jax
import jax.numpy as jnp
from jax import lax
from jax.experimental import pallas as pl
from jax.experimental.pallas import tpu as pltpu
from jax.sharding import PartitionSpec as P

HEAD_WIDTH = 128
DOC_BLKS = 4
MESH = pl.DeviceIdType.MESH
NEG = -1e30


def kernel(n, q_hbm, k_hbm, v_hbm, doc_hbm, o_hbm,
           qbuf, kv, docs, qcol, bias, mref, lref, acc, obuf,
           qsem, loadsem, docsem, docsend, docrecv, send, recv, osem):
    rows = q_hbm.shape[0]
    kv_heads = k_hbm.shape[1] // HEAD_WIDTH
    heads = q_hbm.shape[1] // HEAD_WIDTH
    group = heads // kv_heads
    chunks = 2 * kv_heads
    scale = math.log2(math.e) / math.sqrt(HEAD_WIDTH)

    me = lax.axis_index("blk")
    core = lax.rem(me, 2)
    pair = me // 2
    pairs = n // 2

    def load(i):
        src = (k_hbm, v_hbm)[i % 2].at[:, pl.ds((i // 2) * HEAD_WIDTH, HEAD_WIDTH)]
        return pltpu.make_async_copy(src, kv.at[0, i], loadsem.at[i])

    def load_q(h):
        return pltpu.make_async_copy(q_hbm.at[:, pl.ds(h * HEAD_WIDTH, HEAD_WIDTH)], qbuf.at[h], qsem.at[h])

    load_doc = pltpu.make_async_copy(doc_hbm, docs.at[0], docsem)
    for i in range(chunks):
        load(i).start()
    load_doc.start()
    for h in range(heads):
        load_q(h).start()

    barrier = pltpu.get_barrier_semaphore()
    for o in range(1, DOC_BLKS + 1):
        @pl.when(me + o < n)
        def _():
            pl.semaphore_signal(barrier, inc=1, device_id={"blk": me + o}, device_id_type=MESH)

        @pl.when(me >= o)
        def _():
            pl.semaphore_signal(barrier, inc=1, device_id={"blk": me - o}, device_id_type=MESH)
    pl.semaphore_wait(barrier, jnp.minimum(me, DOC_BLKS) + jnp.minimum(n - 1 - me, DOC_BLKS))

    def doc_copy(o):
        return pltpu.make_async_remote_copy(
            src_ref=docs.at[0], dst_ref=docs.at[o], send_sem=docsend.at[o], recv_sem=docrecv.at[o],
            device_id={"blk": me + o}, device_id_type=MESH)

    def copy(src_slot, dst_slot, i, step):
        return pltpu.make_async_remote_copy(
            src_ref=kv.at[src_slot, i], dst_ref=kv.at[dst_slot, i],
            send_sem=send.at[src_slot, dst_slot, i], recv_sem=recv.at[dst_slot, i],
            device_id={"blk": me + step}, device_id_type=MESH)

    far = me + 4 < n
    relayed_source = (lax.rem(pair, 4) == 1) & (pair + 2 < pairs)
    near = (me + 2 < n) & jnp.logical_not(relayed_source)
    relays = lax.rem(pair, 4) == 3
    late = (lax.rem(pair, 4) == 2) & (pair + 1 < pairs)
    has4 = me >= 4
    has2 = me >= 2
    own_flows = [(far, 0, 4, 4), (near, 0, 2, 2), (core == 0, 0, 1, 1)]
    four_flows = [(has4 & relays, 4, 2, -2), (has4 & (core == 1), 4, 3, -1)]
    two_flows = [(has2 & (core == 0), 2, 3, 1), (has2 & (core == 1), 2, 1, -1)]

    def start(flows, i):
        for cond, s, d, step in flows:
            @pl.when(cond)
            def _():
                copy(s, d, i, step).start()

    def arrived(slot, i):
        copy(0, slot, i, slot).wait_recv()

    load_doc.wait()
    for o in range(1, DOC_BLKS + 1):
        @pl.when(me + o < n)
        def _():
            doc_copy(o).start()
    for i in range(chunks):
        load(i).wait()
        start(own_flows, i)

    qcol[...] = jnp.broadcast_to(docs[0, 0:1, :], (HEAD_WIDTH, rows)).T

    def make_bias(o):
        for c in range(rows // HEAD_WIDTH):
            cols = slice(c * HEAD_WIDTH, (c + 1) * HEAD_WIDTH)
            ok = qcol[...] == docs[o, 0:1, cols]
            if o == 0:
                r = lax.broadcasted_iota(jnp.int32, (rows, HEAD_WIDTH), 0)
                s = lax.broadcasted_iota(jnp.int32, (rows, HEAD_WIDTH), 1) + c * HEAD_WIDTH
                ok = ok & (s <= r)
            bias[o, :, cols] = jnp.where(ok, 0.0, NEG)

    def fold(x, op):
        out = x[:, :HEAD_WIDTH]
        for c in range(1, x.shape[1] // HEAD_WIDTH):
            out = op(out, x[:, c * HEAD_WIDTH:(c + 1) * HEAD_WIDTH])
        return out

    def attend(o, g):
        for j in range(group):
            h = g * group + j
            if o == 0:
                load_q(h).wait()
            s = lax.dot_general(qbuf[h], kv[o, 2 * g], (((1,), (1,)), ((), ())),
                                preferred_element_type=jnp.float32)
            s = s + bias[o]
            m = jnp.max(s, axis=-1, keepdims=True)
            if o > 0:
                old = mref[h][:, :1]
                m = jnp.maximum(m, old)
                alpha = jnp.exp2((old - m) * scale)
            w = jnp.exp2((s - m) * scale)
            l = fold(w, jnp.add)
            a = jnp.dot(w.astype(jnp.bfloat16), kv[o, 2 * g + 1], preferred_element_type=jnp.float32)
            if o > 0:
                l = l + lref[h] * alpha
                a = a + acc[h] * alpha
            mref[h] = jnp.broadcast_to(m, (rows, HEAD_WIDTH))
            lref[h] = l
            acc[h] = a

    make_bias(0)
    for g in range(kv_heads):
        attend(0, g)

    for o in range(1, DOC_BLKS + 1):
        @pl.when(me >= o)
        def _():
            doc_copy(o).wait_recv()
            make_bias(o)

    @pl.when(core == 1)
    def _():
        for i in range(chunks):
            arrived(1, i)
        for g in range(kv_heads):
            attend(1, g)

    def take(cond, slot, flows, i):
        @pl.when(cond)
        def _():
            arrived(slot, i)
        start(flows(i), i) if callable(flows) else start(flows, i)

    prompt2 = has2 & jnp.logical_not(late)
    late2 = has2 & late

    def with_cond(cond, flows):
        return [(cond & c, s, d, step) for c, s, d, step in flows]

    for g in range(kv_heads):
        for i in (2 * g, 2 * g + 1):
            take(has4, 4, four_flows, i)
            take(prompt2, 2, with_cond(prompt2, two_flows), i)

        @pl.when(has4)
        def _():
            attend(4, g)

    for g in range(kv_heads):
        for i in (2 * g, 2 * g + 1):
            take(late2, 2, with_cond(late2, two_flows), i)

        @pl.when(has2)
        def _():
            attend(2, g)

    @pl.when(me >= 3)
    def _():
        for g in range(kv_heads):
            for i in (2 * g, 2 * g + 1):
                arrived(3, i)
            attend(3, g)

    @pl.when((core == 0) & (me >= 1))
    def _():
        for g in range(kv_heads):
            for i in (2 * g, 2 * g + 1):
                arrived(1, i)
            attend(1, g)

    def store(h):
        return pltpu.make_async_copy(obuf.at[h], o_hbm.at[:, pl.ds(h * HEAD_WIDTH, HEAD_WIDTH)], osem.at[h])

    for h in range(heads):
        total = jnp.sum(lref[h], axis=-1, keepdims=True)
        obuf[h] = (acc[h] / total).astype(obuf.dtype)
        store(h).start()

    for o in range(1, DOC_BLKS + 1):
        @pl.when(me + o < n)
        def _():
            doc_copy(o).wait_send()
    for cond, s, d, step in own_flows + four_flows + two_flows:
        @pl.when(cond)
        def _():
            for i in range(chunks):
                copy(s, d, i, step).wait_send()
    for h in range(heads):
        store(h).wait()


def shards(n, queries, keys, values, doc_ids):
    rows = queries.shape[0]
    heads = queries.shape[1] // HEAD_WIDTH
    chunks = 2 * (keys.shape[1] // HEAD_WIDTH)
    slots = DOC_BLKS + 1
    any_spec = pl.BlockSpec(memory_space=pl.ANY)
    stat = pltpu.VMEM((heads, rows, HEAD_WIDTH), jnp.float32)
    return pl.pallas_call(
        functools.partial(kernel, n),
        out_shape=jax.ShapeDtypeStruct(queries.shape, jnp.bfloat16),
        in_specs=[any_spec] * 4,
        out_specs=any_spec,
        scratch_shapes=[
            pltpu.VMEM((heads, rows, HEAD_WIDTH), jnp.bfloat16),
            pltpu.VMEM((slots, chunks, rows, HEAD_WIDTH), jnp.bfloat16),
            pltpu.VMEM((slots, 1, rows), jnp.int32),
            pltpu.VMEM((rows, HEAD_WIDTH), jnp.int32),
            pltpu.VMEM((slots, rows, rows), jnp.float32),
            stat, stat, stat,
            pltpu.VMEM((heads, rows, HEAD_WIDTH), jnp.bfloat16),
            pltpu.SemaphoreType.DMA((heads,)),
            pltpu.SemaphoreType.DMA((chunks,)),
            pltpu.SemaphoreType.DMA,
            pltpu.SemaphoreType.DMA((slots,)),
            pltpu.SemaphoreType.DMA((slots,)),
            pltpu.SemaphoreType.DMA((slots, slots, chunks)),
            pltpu.SemaphoreType.DMA((slots, chunks)),
            pltpu.SemaphoreType.DMA((heads,)),
        ],
        compiler_params=pltpu.CompilerParams(collective_id=0, has_side_effects=True),
    )(queries, keys, values, doc_ids.reshape(1, rows))


def solution(mesh):
    return jax.shard_map(
        functools.partial(shards, mesh.shape["blk"]),
        mesh=mesh,
        in_specs=(P("blk", "heads"), P("blk", "heads"), P("blk", "heads"), P("blk")),
        out_specs=P("blk", "heads"),
        check_vma=False,
    )
```

```python
import functools
import math

import jax
import jax.numpy as jnp
from jax import lax
from jax.experimental import pallas as pl
from jax.experimental.pallas import tpu as pltpu
from jax.sharding import PartitionSpec as P

HEAD_WIDTH = 128
DOC_BLKS = 4
MESH = pl.DeviceIdType.MESH
NEG = -1e30


def kernel(n, q_hbm, k_hbm, v_hbm, doc_hbm, o_ref,
           qbuf, kv, docs, bias, mref, lref, acc,
           qsem, loadsem, docsem, docsend, docrecv, send, recv):
    rows = q_hbm.shape[0]
    kv_heads = k_hbm.shape[1] // HEAD_WIDTH
    heads = q_hbm.shape[1] // HEAD_WIDTH
    group = heads // kv_heads
    chunks = 2 * kv_heads
    scale = math.log2(math.e) / math.sqrt(HEAD_WIDTH)

    me = lax.axis_index("blk")
    core = lax.rem(me, 2)
    pair = me // 2
    pairs = n // 2

    def load(i):
        src = (k_hbm, v_hbm)[i % 2].at[:, pl.ds((i // 2) * HEAD_WIDTH, HEAD_WIDTH)]
        return pltpu.make_async_copy(src, kv.at[0, i], loadsem.at[i])

    def load_q(h):
        return pltpu.make_async_copy(q_hbm.at[:, pl.ds(h * HEAD_WIDTH, HEAD_WIDTH)], qbuf.at[h], qsem.at[h])

    load_doc = pltpu.make_async_copy(doc_hbm, docs.at[0], docsem)
    for i in range(chunks):
        load(i).start()
    load_doc.start()
    for h in range(heads):
        load_q(h).start()

    barrier = pltpu.get_barrier_semaphore()
    for o in range(1, DOC_BLKS + 1):
        @pl.when(me + o < n)
        def _():
            pl.semaphore_signal(barrier, inc=1, device_id={"blk": me + o}, device_id_type=MESH)

        @pl.when(me >= o)
        def _():
            pl.semaphore_signal(barrier, inc=1, device_id={"blk": me - o}, device_id_type=MESH)
    pl.semaphore_wait(barrier, jnp.minimum(me, DOC_BLKS) + jnp.minimum(n - 1 - me, DOC_BLKS))

    def doc_copy(o):
        return pltpu.make_async_remote_copy(
            src_ref=docs.at[0], dst_ref=docs.at[o], send_sem=docsend.at[o], recv_sem=docrecv.at[o],
            device_id={"blk": me + o}, device_id_type=MESH)

    def copy(src_slot, dst_slot, i, step):
        return pltpu.make_async_remote_copy(
            src_ref=kv.at[src_slot, i], dst_ref=kv.at[dst_slot, i],
            send_sem=send.at[src_slot, dst_slot, i], recv_sem=recv.at[dst_slot, i],
            device_id={"blk": me + step}, device_id_type=MESH)

    far = me + 4 < n
    relayed_source = (lax.rem(pair, 4) == 1) & (pair + 2 < pairs)
    near = (me + 2 < n) & jnp.logical_not(relayed_source)
    relays = lax.rem(pair, 4) == 3
    late = (lax.rem(pair, 4) == 2) & (pair + 1 < pairs)
    has4 = me >= 4
    has2 = me >= 2
    own_flows = [(far, 0, 4, 4), (near, 0, 2, 2), (core == 0, 0, 1, 1)]
    four_flows = [(has4 & relays, 4, 2, -2), (has4 & (core == 1), 4, 3, -1)]
    two_flows = [(has2 & (core == 0), 2, 3, 1), (has2 & (core == 1), 2, 1, -1)]

    def start(flows, i):
        for cond, s, d, step in flows:
            @pl.when(cond)
            def _():
                copy(s, d, i, step).start()

    def arrived(slot, i):
        pltpu.make_async_remote_copy(
            src_ref=kv.at[0, i], dst_ref=kv.at[slot, i], send_sem=send.at[0, 1, i], recv_sem=recv.at[slot, i],
            device_id={"blk": lax.rem(me + 1, n)}, device_id_type=MESH).wait_recv()

    load_doc.wait()
    for o in range(1, DOC_BLKS + 1):
        @pl.when(me + o < n)
        def _():
            doc_copy(o).start()
    for i in range(chunks):
        load(i).wait()
        start(own_flows, i)

    def column(row):
        return jnp.broadcast_to(row, (HEAD_WIDTH, rows)).T

    def make_bias(o):
        key_docs = column(docs[o, 0:1, :])
        for c in range(rows // HEAD_WIDTH):
            cols = slice(c * HEAD_WIDTH, (c + 1) * HEAD_WIDTH)
            ok = key_docs == docs[0, 0:1, cols]
            if o == 0:
                s = lax.broadcasted_iota(jnp.int32, (rows, HEAD_WIDTH), 0)
                r = lax.broadcasted_iota(jnp.int32, (rows, HEAD_WIDTH), 1) + c * HEAD_WIDTH
                ok = ok & (s <= r)
            bias[o, :, cols] = jnp.where(ok, 0.0, NEG)

    def own(o):
        return isinstance(o, int) and o == 0

    def scores(o, h):
        g = h // group
        if own(o):
            load_q(h).wait()
        s = lax.dot_general(kv[o, 2 * g], qbuf[h], (((1,), (1,)), ((), ())),
                            preferred_element_type=jnp.float32)
        s = s + bias[o]
        return s, jnp.max(s, axis=0, keepdims=True)

    def weigh(o, h, s, m, values_t):
        if not own(o):
            old = mref[h]
            m = jnp.maximum(m, old)
            alpha = jnp.exp2((old - m) * scale)
        w = jnp.exp2(s * scale - m * scale)
        l = jnp.sum(w, axis=0, keepdims=True)
        a = jnp.dot(values_t, w.astype(jnp.bfloat16), preferred_element_type=jnp.float32)
        if not own(o):
            l = l + lref[h] * alpha
            a = a + acc[h] * alpha
        mref[h] = m
        lref[h] = l
        acc[h] = a

    def attend(o, groups):
        todo = [h for g in groups for h in range(g * group, (g + 1) * group)]
        values_t = {g: kv[o, 2 * g + 1].T for g in groups}
        held = scores(o, todo[0])
        for k, h in enumerate(todo):
            ahead = scores(o, todo[k + 1]) if k + 1 < len(todo) else None
            weigh(o, h, *held, values_t[h // group])
            held = ahead

    make_bias(0)
    attend(0, range(kv_heads))

    for o in range(1, DOC_BLKS + 1):
        @pl.when(me >= o)
        def _():
            doc_copy(o).wait_recv()
            make_bias(o)

    @pl.when(core == 1)
    def _():
        for i in range(chunks):
            arrived(1, i)
        attend(1, range(kv_heads))

    def take(cond, slot, flows, i):
        @pl.when(cond)
        def _():
            arrived(slot, i)
        start(flows(i), i) if callable(flows) else start(flows, i)

    prompt2 = has2 & jnp.logical_not(late)
    late2 = has2 & late

    def with_cond(cond, flows):
        return [(cond & c, s, d, step) for c, s, d, step in flows]

    for g in range(kv_heads):
        for i in (2 * g, 2 * g + 1):
            take(has4, 4, four_flows, i)
            take(prompt2, 2, with_cond(prompt2, two_flows), i)

        @pl.when(has4)
        def _():
            attend(4, [g])

        @pl.when(has4 & (core == 0))
        def _():
            for i in (2 * g, 2 * g + 1):
                arrived(3, i)
            attend(3, [g])

    last = jnp.where(core == 0, 1, 3)
    for g in range(kv_heads):
        for i in (2 * g, 2 * g + 1):
            take(late2, 2, with_cond(late2, two_flows), i)

        @pl.when(has2)
        def _():
            attend(2, [g])
            for i in (2 * g, 2 * g + 1):
                arrived(last, i)
            attend(last, [g])

    for h in range(heads):
        o_ref[:, h * HEAD_WIDTH:(h + 1) * HEAD_WIDTH] = (acc[h] / lref[h]).T.astype(o_ref.dtype)

    for o in range(1, DOC_BLKS + 1):
        @pl.when(me + o < n)
        def _():
            doc_copy(o).wait_send()
    for cond, s, d, step in own_flows + four_flows + two_flows:
        @pl.when(cond)
        def _():
            for i in range(chunks):
                copy(s, d, i, step).wait_send()


def shards(n, queries, keys, values, doc_ids):
    rows = queries.shape[0]
    heads = queries.shape[1] // HEAD_WIDTH
    chunks = 2 * (keys.shape[1] // HEAD_WIDTH)
    slots = DOC_BLKS + 1
    hbm_spec = pl.BlockSpec(memory_space=pltpu.HBM)
    stat = pltpu.VMEM((heads, 1, rows), jnp.float32)
    return pl.pallas_call(
        functools.partial(kernel, n),
        out_shape=pltpu.VMEM(queries.shape, jnp.bfloat16),
        in_specs=[hbm_spec] * 4,
        out_specs=pl.BlockSpec(memory_space=pltpu.VMEM),
        scratch_shapes=[
            pltpu.VMEM((heads, rows, HEAD_WIDTH), jnp.bfloat16),
            pltpu.VMEM((slots, chunks, rows, HEAD_WIDTH), jnp.bfloat16),
            pltpu.VMEM((slots, 1, rows), jnp.int32),
            pltpu.VMEM((slots, rows, rows), jnp.float32),
            stat, stat,
            pltpu.VMEM((heads, HEAD_WIDTH, rows), jnp.float32),
            pltpu.SemaphoreType.DMA((heads,)),
            pltpu.SemaphoreType.DMA((chunks,)),
            pltpu.SemaphoreType.DMA,
            pltpu.SemaphoreType.DMA((slots,)),
            pltpu.SemaphoreType.DMA((slots,)),
            pltpu.SemaphoreType.DMA((slots, slots, chunks)),
            pltpu.SemaphoreType.DMA((slots, chunks)),
        ],
        compiler_params=pltpu.CompilerParams(collective_id=0, has_side_effects=True,
                                             vmem_limit_bytes=24 * 2**20),
    )(*(pltpu.with_memory_space_constraint(x, pltpu.HBM) for x in (queries, keys, values, doc_ids.reshape(1, rows))))


def solution(mesh):
    return jax.shard_map(
        functools.partial(shards, mesh.shape["blk"]),
        mesh=mesh,
        in_specs=(P("blk", "heads"), P("blk", "heads"), P("blk", "heads"), P("blk")),
        out_specs=P("blk", "heads"),
        check_vma=False,
    )
```

```python
import functools
import math

import jax
import jax.numpy as jnp
from jax import lax
from jax.experimental import pallas as pl
from jax.experimental.pallas import tpu as pltpu
from jax.sharding import PartitionSpec as P

HEAD_WIDTH = 128
DOC_BLKS = 4
MESH = pl.DeviceIdType.MESH
NEG = -1e30


def kernel(n, q_hbm, k_hbm, v_hbm, doc_hbm, o_ref,
           qbuf, kv, docs, bias, mref, lref, acc,
           qsem, loadsem, docsem, docsend, docrecv, send, recv):
    rows = q_hbm.shape[0]
    kv_heads = k_hbm.shape[1] // HEAD_WIDTH
    heads = q_hbm.shape[1] // HEAD_WIDTH
    group = heads // kv_heads
    chunks = 2 * kv_heads
    scale = math.log2(math.e) / math.sqrt(HEAD_WIDTH)

    me = lax.axis_index("blk")
    core = lax.rem(me, 2)
    pair = me // 2
    pairs = n // 2

    def load(i):
        src = (k_hbm, v_hbm)[i % 2].at[:, pl.ds((i // 2) * HEAD_WIDTH, HEAD_WIDTH)]
        return pltpu.make_async_copy(src, kv.at[0, i], loadsem.at[i])

    def load_q(h):
        return pltpu.make_async_copy(q_hbm.at[:, pl.ds(h * HEAD_WIDTH, HEAD_WIDTH)], qbuf.at[h], qsem.at[h])

    load_doc = pltpu.make_async_copy(doc_hbm, docs.at[0], docsem)
    for i in range(chunks):
        load(i).start()
    load_doc.start()
    for h in range(heads):
        load_q(h).start()

    barrier = pltpu.get_barrier_semaphore()
    for o in range(1, DOC_BLKS + 1):
        @pl.when(me + o < n)
        def _():
            pl.semaphore_signal(barrier, inc=1, device_id={"blk": me + o}, device_id_type=MESH)

        @pl.when(me >= o)
        def _():
            pl.semaphore_signal(barrier, inc=1, device_id={"blk": me - o}, device_id_type=MESH)
    pl.semaphore_wait(barrier, jnp.minimum(me, DOC_BLKS) + jnp.minimum(n - 1 - me, DOC_BLKS))

    def doc_copy(o):
        return pltpu.make_async_remote_copy(
            src_ref=docs.at[0], dst_ref=docs.at[o], send_sem=docsend.at[o], recv_sem=docrecv.at[o],
            device_id={"blk": me + o}, device_id_type=MESH)

    def copy(src_slot, dst_slot, i, step):
        return pltpu.make_async_remote_copy(
            src_ref=kv.at[src_slot, i], dst_ref=kv.at[dst_slot, i],
            send_sem=send.at[src_slot, dst_slot, i], recv_sem=recv.at[dst_slot, i],
            device_id={"blk": me + step}, device_id_type=MESH)

    far = me + 4 < n
    relayed_source = (lax.rem(pair, 4) == 1) & (pair + 2 < pairs)
    skips = (me + 2 < n) & relayed_source
    near = (me + 2 < n) & jnp.logical_not(relayed_source)
    relays = lax.rem(pair, 4) == 3
    late = (lax.rem(pair, 4) == 2) & (pair + 1 < pairs)
    has4 = me >= 4
    has2 = me >= 2
    own_flows = [(far, 0, 4, 4), (near, 0, 2, 2), (core == 0, 0, 1, 1)]
    four_flows = [(has4 & relays, 4, 2, -2), (has4 & (core == 1), 4, 3, -1)]
    two_flows = [(has2 & (core == 0), 2, 3, 1), (has2 & (core == 1), 2, 1, -1)]

    def start(flows, i):
        for cond, s, d, step in flows:
            if step == -2 and i == chunks - 1:
                continue
            @pl.when(cond)
            def _():
                copy(s, d, i, step).start()

    def arrived(slot, i):
        pltpu.make_async_remote_copy(
            src_ref=kv.at[0, i], dst_ref=kv.at[slot, i], send_sem=send.at[0, 1, i], recv_sem=recv.at[slot, i],
            device_id={"blk": lax.rem(me + 1, n)}, device_id_type=MESH).wait_recv()

    for i in range(chunks):
        load(i).wait()
        start(own_flows, i)
        if i == 0:
            load_doc.wait()
            for o in range(1, DOC_BLKS + 1):
                @pl.when(me + o < n)
                def _():
                    doc_copy(o).start()

    def column(row):
        return jnp.broadcast_to(row, (HEAD_WIDTH, rows)).T

    def make_bias(o):
        key_docs = column(docs[o, 0:1, :])
        for c in range(rows // HEAD_WIDTH):
            cols = slice(c * HEAD_WIDTH, (c + 1) * HEAD_WIDTH)
            ok = key_docs == docs[0, 0:1, cols]
            if o == 0:
                s = lax.broadcasted_iota(jnp.int32, (rows, HEAD_WIDTH), 0)
                r = lax.broadcasted_iota(jnp.int32, (rows, HEAD_WIDTH), 1) + c * HEAD_WIDTH
                ok = ok & (s <= r)
            bias[o, :, cols] = jnp.where(ok, 0.0, NEG)

    def own(o):
        return isinstance(o, int) and o == 0

    def scores(o, h):
        g = h // group
        if own(o):
            load_q(h).wait()
        s = lax.dot_general(kv[o, 2 * g], qbuf[h], (((1,), (1,)), ((), ())),
                            preferred_element_type=jnp.float32)
        s = s + bias[o]
        return s, jnp.max(s, axis=0, keepdims=True)

    def weigh(o, h, s, m, values_t):
        if not own(o):
            old = mref[h]
            m = jnp.maximum(m, old)
            alpha = jnp.exp2((old - m) * scale)
        w = jnp.exp2(s * scale - m * scale)
        l = jnp.sum(w, axis=0, keepdims=True)
        a = jnp.dot(values_t, w.astype(jnp.bfloat16), preferred_element_type=jnp.float32)
        if not own(o):
            l = l + lref[h] * alpha
            a = a + acc[h] * alpha
        mref[h] = m
        lref[h] = l
        acc[h] = a

    def attend(o, groups):
        todo = [h for g in groups for h in range(g * group, (g + 1) * group)]
        values_t = {g: kv[o, 2 * g + 1].T for g in groups}
        held = scores(o, todo[0])
        for k, h in enumerate(todo):
            ahead = scores(o, todo[k + 1]) if k + 1 < len(todo) else None
            weigh(o, h, *held, values_t[h // group])
            held = ahead

    make_bias(0)
    attend(0, range(kv_heads))

    def receive_docs(o):
        @pl.when(me >= o)
        def _():
            doc_copy(o).wait_recv()
            make_bias(o)

    receive_docs(1)
    @pl.when(core == 1)
    def _():
        for i in range(chunks):
            arrived(1, i)
        attend(1, range(kv_heads))

    def take(cond, slot, flows, i):
        @pl.when(cond)
        def _():
            arrived(slot, i)
        start(flows(i), i) if callable(flows) else start(flows, i)

    prompt2 = has2 & jnp.logical_not(late)
    late2 = has2 & late

    def with_cond(cond, flows):
        return [(cond & c, s, d, step) for c, s, d, step in flows]

    for o in range(2, DOC_BLKS + 1):
        receive_docs(o)

    for g in range(kv_heads):
        for i in (2 * g, 2 * g + 1):
            take(has4, 4, four_flows, i)
            take(prompt2, 2, with_cond(prompt2, two_flows), i)

        if g == 0:
            @pl.when(skips)
            def _():
                copy(0, 2, chunks - 1, 2).start()

        @pl.when(has4)
        def _():
            attend(4, [g])

        @pl.when(has4 & (core == 0))
        def _():
            for i in (2 * g, 2 * g + 1):
                arrived(3, i)
            attend(3, [g])

    last = jnp.where(core == 0, 1, 3)
    for g in range(kv_heads):
        for i in (2 * g, 2 * g + 1):
            take(late2, 2, with_cond(late2, two_flows), i)

        @pl.when(has2)
        def _():
            attend(2, [g])
            for i in (2 * g, 2 * g + 1):
                arrived(last, i)
            attend(last, [g])

    @pl.when(skips)
    def _():
        copy(0, 2, chunks - 1, 2).wait_send()

    for h in range(heads):
        o_ref[:, h * HEAD_WIDTH:(h + 1) * HEAD_WIDTH] = (acc[h] / lref[h]).T.astype(o_ref.dtype)

    for o in range(1, DOC_BLKS + 1):
        @pl.when(me + o < n)
        def _():
            doc_copy(o).wait_send()
    for cond, s, d, step in own_flows + four_flows + two_flows:
        @pl.when(cond)
        def _():
            for i in range(chunks - (step == -2)):
                copy(s, d, i, step).wait_send()


def shards(n, queries, keys, values, doc_ids):
    rows = queries.shape[0]
    heads = queries.shape[1] // HEAD_WIDTH
    chunks = 2 * (keys.shape[1] // HEAD_WIDTH)
    slots = DOC_BLKS + 1
    hbm_spec = pl.BlockSpec(memory_space=pltpu.HBM)
    stat = pltpu.VMEM((heads, 1, rows), jnp.float32)
    return pl.pallas_call(
        functools.partial(kernel, n),
        out_shape=pltpu.VMEM(queries.shape, jnp.bfloat16),
        in_specs=[hbm_spec] * 4,
        out_specs=pl.BlockSpec(memory_space=pltpu.VMEM),
        scratch_shapes=[
            pltpu.VMEM((heads, rows, HEAD_WIDTH), jnp.bfloat16),
            pltpu.VMEM((slots, chunks, rows, HEAD_WIDTH), jnp.bfloat16),
            pltpu.VMEM((slots, 1, rows), jnp.int32),
            pltpu.VMEM((slots, rows, rows), jnp.float32),
            stat, stat,
            pltpu.VMEM((heads, HEAD_WIDTH, rows), jnp.float32),
            pltpu.SemaphoreType.DMA((heads,)),
            pltpu.SemaphoreType.DMA((chunks,)),
            pltpu.SemaphoreType.DMA,
            pltpu.SemaphoreType.DMA((slots,)),
            pltpu.SemaphoreType.DMA((slots,)),
            pltpu.SemaphoreType.DMA((slots, slots, chunks)),
            pltpu.SemaphoreType.DMA((slots, chunks)),
        ],
        compiler_params=pltpu.CompilerParams(collective_id=0, has_side_effects=True,
                                             vmem_limit_bytes=24 * 2**20),
    )(*(pltpu.with_memory_space_constraint(x, pltpu.HBM) for x in (queries, keys, values, doc_ids.reshape(1, rows))))


def solution(mesh):
    return jax.shard_map(
        functools.partial(shards, mesh.shape["blk"]),
        mesh=mesh,
        in_specs=(P("blk", "heads"), P("blk", "heads"), P("blk", "heads"), P("blk")),
        out_specs=P("blk", "heads"),
        check_vma=False,
    )
```
